32 devices in a mesh: head: 8 (over z, y), ctx: 4 (over x, core).
Axes of the slice: x: 2, y: 2, z: 4, core: 2. Of those that a mesh axis runs over, the one named last changes fastest.
Arguments:
- query: bfloat16 [3072, 4096], P(('ctx', 'head')), may hold values from -8 to 8
- key: bfloat16 [3072, 2048], P(('ctx', 'head')), may hold values from -8 to 8
- value: bfloat16 [3072, 2048], P(('ctx', 'head')), may hold values from -8 to 8
- block_order: int32 [8], replicated, may hold values from 0 to 7, each once
Outputs:
- attended: bfloat16 [3072, 4096], P('ctx', 'head')
The draws below stay inside these ranges and needn't reach their ends.
Inputs may be any that keep to these rules, and one draw needn't show every extreme that they name: `block_order`: each storage block index 0 to 7 appears exactly once.
All inputs are finite; a program needn't handle non-finite values.
Results may differ from the reference program's by a relative error of at most 0.0049.
Values may be sent and summed in bfloat16 or wider, within the bound.
A program may use at most 128 MiB of HBM per device.

```python
import jax
import jax.numpy as jnp
from jax import lax

HQ = 32
KEY_HEADS = 16
HEAD_WIDTH = 128
QUERY_PER_KEY = 2
TOKEN_COUNT = 3072
BLK = 384
BLOCKS = 8


def levels(stream_key, dims, split, low, high):
    factor_of, own = 1.0, jax.random.fold_in(stream_key, 6)
    for position, shards_of in split:
        draws = jnp.exp(jax.random.uniform(jax.random.fold_in(own, position), (shards_of,), jnp.float32, low / len(split), high / len(split)))
        factor_of = factor_of * jnp.repeat(draws, dims[position] // shards_of).reshape([-1 if axis == position else 1 for axis in range(len(dims))])
    return factor_of


def scatter_about(stream_key, shape, spread, most, cuts=(), held_as=jnp.bfloat16):
    values = spread * jax.random.normal(stream_key, shape, jnp.float32)
    if cuts:
        values = values * levels(stream_key, shape, cuts, -0.22, 0.18)
    return jnp.clip(values, -most, most).astype(held_as)


def setup_inputs(seed: int = 0) -> dict:
    streams_of = jax.random.split(jax.random.key(seed), 5)
    query = scatter_about(streams_of[0], (TOKEN_COUNT, HQ * HEAD_WIDTH), 1.5, 8.0, ((0, 32),))
    key = scatter_about(streams_of[1], (TOKEN_COUNT, KEY_HEADS * HEAD_WIDTH), 1.0, 8.0, ((0, 32),))
    value = scatter_about(streams_of[2], (TOKEN_COUNT, KEY_HEADS * HEAD_WIDTH), 1.0, 8.0, ((0, 32),))
    block_order = jax.random.permutation(streams_of[3], BLOCKS).astype(jnp.int32)
    return {"query": query, "key": key, "value": value, "block_order": block_order}


query_scale = 1.0 / 12.0
softcap_limit = 50.0


def head_block(query_rows, key_rows, value_rows, query_pos, key_pos):
    scores = jnp.einsum('rgd,kd->grk', query_rows.astype(jnp.float32), key_rows.astype(jnp.float32)) * query_scale
    capped = softcap_limit * jnp.tanh(scores / softcap_limit)
    visible = key_pos[None, :] <= query_pos[:, None]
    weights = jnp.where(visible[None], jnp.exp(capped), jnp.zeros_like(capped))
    denominator = jnp.sum(weights, axis=-1)
    rounded = lax.optimization_barrier(weights.astype(jnp.bfloat16)).astype(jnp.float32)
    numerator = jnp.einsum('grk,kd->grd', rounded, value_rows.astype(jnp.float32))
    return jnp.transpose(numerator / denominator[..., None], (1, 0, 2))


def reference(query, key, value, block_order):
    sequence_length = query.shape[0]
    positions = (block_order[:, None].astype(jnp.int32) * BLK + jnp.arange(BLK, dtype=jnp.int32)[None, :]).reshape(sequence_length)
    row_block = 2 * BLK
    block_count = sequence_length // row_block
    query_rows = query.reshape(sequence_length, KEY_HEADS, QUERY_PER_KEY, HEAD_WIDTH)
    key_rows = key.reshape(sequence_length, KEY_HEADS, HEAD_WIDTH)
    value_rows = value.reshape(sequence_length, KEY_HEADS, HEAD_WIDTH)
    columns = []
    for key_value_head in range(KEY_HEADS):
        def one_block(pieces, key_value_head=key_value_head):
            return head_block(pieces[0], key_rows[:, key_value_head], value_rows[:, key_value_head], pieces[1], positions)
        blocks = lax.map(one_block, (query_rows[:, key_value_head].reshape(block_count, row_block, QUERY_PER_KEY, HEAD_WIDTH), positions.reshape(block_count, row_block)))
        columns.append(blocks.reshape(sequence_length, QUERY_PER_KEY * HEAD_WIDTH))
    return jnp.concatenate(columns, axis=1).astype(jnp.bfloat16)
```

```python
import functools
import math

import jax
import jax.numpy as jnp
from jax import lax
from jax.experimental import pallas as pl
from jax.experimental.pallas import tpu as pltpu
from jax.sharding import PartitionSpec as P

HEAD_WIDTH = 128
MESH = pl.DeviceIdType.MESH
CAP = 50.0
IN_SCALE = 1.0 / (12.0 * CAP)
OUT_SCALE = CAP * math.log2(math.e)
HIDDEN = -4096.0


def flip(index, step, size):
    out, bit = 0, 1
    while bit < size:
        mine = (index // bit) % 2
        turn = (step // bit) % 2
        out = out + (mine + turn - 2 * mine * turn) * bit
        bit *= 2
    return out


def kernel(
    n_head, n_ctx, pair,
    order, query, key, value, out,
    qbuf, kv, acc,
    q_send, k_send, v_send, q_recv, k_recv, v_recv,
    local_sem, f_send, r_send, f_recv,
):
    me = lax.axis_index("head")
    ctx = lax.axis_index("ctx")
    chip, core = ctx // 2, ctx % 2
    partner = chip * 2 + 1 - core
    chips = n_ctx // 2
    pieces = n_head // pair
    rows = query.shape[0]
    total = rows * n_head
    block = total // 2
    q_cols = query.shape[1] // n_head
    kv_cols = key.shape[1] // n_head
    kv_heads = kv_cols // HEAD_WIDTH
    per_kv = q_cols // kv_cols
    piece_rows = rows * pair
    same_core = [((chip + t) % chips) * 2 + core for t in range(1, chips)]
    peers = [flip(me, j, n_head) for j in range(1, n_head)]

    barrier = pltpu.get_barrier_semaphore()
    for d in peers:
        pl.semaphore_signal(barrier, inc=1, device_id={"head": d}, device_id_type=MESH)
    for c in [partner] + same_core:
        pl.semaphore_signal(barrier, inc=1, device_id={"ctx": c}, device_id_type=MESH)

    def rows_of(s):
        return pl.ds(pl.multiple_of(s * rows, rows), rows)

    def cols_of(s, width):
        return pl.ds(pl.multiple_of(s * width, width), width)

    mine = [
        pltpu.make_async_copy(key.at[:, cols_of(me, kv_cols)], kv.at[ctx, 0, rows_of(me)], local_sem.at[0]),
        pltpu.make_async_copy(value.at[:, cols_of(me, kv_cols)], kv.at[ctx, 1, rows_of(me)], local_sem.at[1]),
        pltpu.make_async_copy(query.at[:, cols_of(me, q_cols)], qbuf.at[rows_of(me)], local_sem.at[2]),
    ]
    for copy in mine:
        copy.start()

    pl.semaphore_wait(barrier, n_head - 1 + chips)

    def to_head(src, width, dst, send, recv, d):
        return pltpu.make_async_remote_copy(
            src_ref=src.at[:, cols_of(d, width)], dst_ref=dst.at[rows_of(me)],
            send_sem=send.at[d], recv_sem=recv.at[me],
            device_id={"head": d}, device_id_type=MESH,
        )

    sends = []
    for d in peers:
        sends.append(to_head(key, kv_cols, kv.at[ctx, 0], k_send, k_recv, d))
        sends.append(to_head(value, kv_cols, kv.at[ctx, 1], v_send, v_recv, d))
    for d in peers:
        sends.append(to_head(query, q_cols, qbuf, q_send, q_recv, d))
    for copy in sends:
        copy.start()

    def arrived(dst, recv, s):
        pltpu.make_async_copy(dst.at[rows_of(s)], dst.at[rows_of(s)], recv.at[s]).wait()

    def piece_ref(c, p):
        return kv.at[c, :, pl.ds(pl.multiple_of(p * piece_rows, piece_rows), piece_rows)]

    def forward(c, p, dest, send):
        return pltpu.make_async_remote_copy(
            src_ref=piece_ref(c, p), dst_ref=piece_ref(c, p),
            send_sem=send, recv_sem=f_recv.at[c, p],
            device_id={"ctx": dest}, device_id_type=MESH,
        )

    def piece_arrived(c, p):
        pltpu.make_async_copy(piece_ref(c, p), piece_ref(c, p), f_recv.at[c, p]).wait()

    passed = []

    def relay(p):
        for c in same_core:
            piece_arrived(c, p)
            copy = forward(c, p, partner, r_send.at[c, p])
            copy.start()
            passed.append(copy)

    home = me // pair
    for step in range(pieces):
        p = flip(home, step, pieces)
        for t in range(pair):
            s = flip(me, step * pair + t, n_head)
            if step == 0 and t == 0:
                mine[0].wait()
                mine[1].wait()
            else:
                arrived(kv.at[ctx, 0], k_recv, s)
                arrived(kv.at[ctx, 1], v_recv, s)
        for dest in same_core + [partner]:
            copy = forward(ctx, p, dest, f_send.at[dest, p])
            copy.start()
            passed.append(copy)
        if step > 0:
            relay(flip(home, step - 1, pieces))
    relay(flip(home, pieces - 1, pieces))
    for t in range(chips):
        c = ((chip + t) % chips) * 2 + 1 - core
        for step in range(pieces):
            piece_arrived(c, flip(home, step, pieces))
    mine[2].wait()

    ones = jnp.ones((total, HEAD_WIDTH), jnp.bfloat16)

    def q_head(g, h):
        span = pl.ds(pl.multiple_of(g * piece_rows, piece_rows), piece_rows)
        return jnp.concatenate(
            [qbuf[span, (h * per_kv + i) * HEAD_WIDTH : (h * per_kv + i + 1) * HEAD_WIDTH] for i in range(per_kv)],
            axis=0,
        )

    def scores_of(g, h, c):
        k = kv[c, 0, :, h * HEAD_WIDTH : (h + 1) * HEAD_WIDTH]
        s = lax.dot_general(q_head(g, h), k, (((1,), (1,)), ((), ())), preferred_element_type=jnp.float32)
        return jnp.tanh(s * IN_SCALE) * OUT_SCALE

    def weighted(w, h, c):
        v = kv[c, 1, :, h * HEAD_WIDTH : (h + 1) * HEAD_WIDTH]
        return jnp.dot(w.astype(jnp.bfloat16), jnp.concatenate([v, ones], axis=1), preferred_element_type=jnp.float32)

    def one_group(step, carry):
        g = flip(home, step, pieces)
        for t in range(pair):
            j = step * pair + t
            s = flip(me, j, n_head)

            @pl.when(j > 0)
            def _():
                arrived(qbuf, q_recv, s)

        first_row = g * piece_rows
        half = first_row // block
        q_block = order[2 * ctx + half]
        q_pos = q_block * block + (first_row - half * block) + lax.broadcasted_iota(jnp.int32, (piece_rows, total), 0)
        col = lax.broadcasted_iota(jnp.int32, (piece_rows, total), 1)
        k_pos = jnp.where(col < block, order[2 * ctx] * block + col, order[2 * ctx + 1] * block + col - block)
        visible = k_pos <= q_pos
        for h in range(kv_heads):
            e = jnp.exp2(scores_of(g, h, ctx)).reshape(per_kv, piece_rows, total)
            w = jnp.where(visible[None], e, 0.0).reshape(per_kv * piece_rows, total)
            acc[h] = weighted(w, h, ctx)

        def other(d, carry):
            c = (ctx + d) % n_ctx
            low = jnp.where(order[2 * c] <= q_block, 0.0, HIDDEN)
            high = jnp.where(order[2 * c + 1] <= q_block, 0.0, HIDDEN)
            for h in range(kv_heads):
                x = scores_of(g, h, c)
                w = jnp.concatenate([jnp.exp2(x[:, :block] + low), jnp.exp2(x[:, block:] + high)], axis=1)
                acc[h] += weighted(w, h, c)
            return carry

        lax.fori_loop(1, n_ctx, other, 0)
        span = pl.ds(pl.multiple_of(first_row, piece_rows), piece_rows)
        for h in range(kv_heads):
            a = acc[h]
            o = (a[:, :HEAD_WIDTH] / a[:, HEAD_WIDTH:]).astype(jnp.bfloat16)
            for i in range(per_kv):
                at = (h * per_kv + i) * HEAD_WIDTH
                out[span, at : at + HEAD_WIDTH] = o[i * piece_rows : (i + 1) * piece_rows]
        return carry

    lax.fori_loop(0, pieces, one_group, 0)
    for copy in sends:
        copy.wait_send()
    for copy in passed:
        copy.wait_send()


def shards(n_head, n_ctx, query, key, value, block_order):
    rows = query.shape[0]
    total = rows * n_head
    q_cols = query.shape[1] // n_head
    kv_cols = key.shape[1] // n_head
    kv_heads = kv_cols // HEAD_WIDTH
    per_kv = q_cols // kv_cols
    pair = 2
    pieces = n_head // pair
    hbm = pl.BlockSpec(memory_space=pltpu.HBM)
    dma = pltpu.SemaphoreType.DMA
    return pl.pallas_call(
        functools.partial(kernel, n_head, n_ctx, pair),
        out_shape=jax.ShapeDtypeStruct((total, q_cols), jnp.bfloat16),
        in_specs=[pl.BlockSpec(memory_space=pltpu.SMEM), hbm, hbm, hbm],
        out_specs=pl.BlockSpec(memory_space=pltpu.VMEM),
        scratch_shapes=[
            pltpu.VMEM((total, q_cols), jnp.bfloat16),
            pltpu.VMEM((n_ctx, 2, total, kv_cols), jnp.bfloat16),
            pltpu.VMEM((kv_heads, per_kv * pair * rows, 2 * HEAD_WIDTH), jnp.float32),
            dma((n_head,)), dma((n_head,)), dma((n_head,)),
            dma((n_head,)), dma((n_head,)), dma((n_head,)),
            dma((3,)),
            dma((n_ctx, pieces)), dma((n_ctx, pieces)), dma((n_ctx, pieces)),
        ],
        compiler_params=pltpu.CompilerParams(
            collective_id=0, has_side_effects=True, vmem_limit_bytes=60 * 1024 * 1024
        ),
    )(block_order, query, key, value)


def solution(mesh):
    placed = (P(("ctx", "head"), None), P(("ctx", "head"), None), P(("ctx", "head"), None), P())
    return jax.shard_map(
        functools.partial(shards, mesh.shape["head"], mesh.shape["ctx"]),
        mesh=mesh, in_specs=placed, out_specs=P("ctx", "head"), check_vma=False,
    )
```

```python
import functools
import math

import jax
import jax.numpy as jnp
from jax import lax
from jax.experimental import pallas as pl
from jax.experimental.pallas import tpu as pltpu
from jax.sharding import PartitionSpec as P

HEAD_WIDTH = 128
MESH = pl.DeviceIdType.MESH
CAP = 50.0
IN_SCALE = 1.0 / (12.0 * CAP)
OUT_SCALE = CAP * math.log2(math.e)
HIDDEN = -4096.0


def flip(index, step, size):
    out, bit = 0, 1
    while bit < size:
        mine = (index // bit) % 2
        turn = (step // bit) % 2
        out = out + (mine + turn - 2 * mine * turn) * bit
        bit *= 2
    return out


def kernel(
    n_head, n_ctx, pair,
    order, query, key, value, out,
    qbuf, kv, acc,
    q_send, k_send, v_send, q_recv, k_recv, v_recv,
    local_sem, f_send, r_send, f_recv,
):
    me = lax.axis_index("head")
    ctx = lax.axis_index("ctx")
    chip, core = ctx // 2, ctx % 2
    partner = chip * 2 + 1 - core
    chips = n_ctx // 2
    pieces = n_head // pair
    rows = query.shape[0]
    total = rows * n_head
    block = total // 2
    q_cols = query.shape[1] // n_head
    kv_cols = key.shape[1] // n_head
    kv_heads = kv_cols // HEAD_WIDTH
    per_kv = q_cols // kv_cols
    piece_rows = rows * pair
    same_core = [((chip + t) % chips) * 2 + core for t in range(1, chips)]
    peers = [flip(me, j, n_head) for j in range(1, n_head)]

    barrier = pltpu.get_barrier_semaphore()
    for d in peers:
        pl.semaphore_signal(barrier, inc=1, device_id={"head": d}, device_id_type=MESH)
    for c in [partner] + same_core:
        pl.semaphore_signal(barrier, inc=1, device_id={"ctx": c}, device_id_type=MESH)

    def rows_of(s):
        return pl.ds(pl.multiple_of(s * rows, rows), rows)

    def cols_of(s, width):
        return pl.ds(pl.multiple_of(s * width, width), width)

    mine = [
        pltpu.make_async_copy(key.at[:, cols_of(me, kv_cols)], kv.at[ctx, 0, rows_of(me)], local_sem.at[0]),
        pltpu.make_async_copy(value.at[:, cols_of(me, kv_cols)], kv.at[ctx, 1, rows_of(me)], local_sem.at[1]),
        pltpu.make_async_copy(query.at[:, cols_of(me, q_cols)], qbuf.at[rows_of(me)], local_sem.at[2]),
    ]
    for copy in mine:
        copy.start()

    pl.semaphore_wait(barrier, n_head - 1 + chips)

    def to_head(src, width, dst, send, recv, d):
        return pltpu.make_async_remote_copy(
            src_ref=src.at[:, cols_of(d, width)], dst_ref=dst.at[rows_of(me)],
            send_sem=send.at[d], recv_sem=recv.at[me],
            device_id={"head": d}, device_id_type=MESH,
        )

    near = n_head // 2
    sends = []
    for some in (peers[: near - 1], peers[near - 1 :]):
        for d in some:
            sends.append(to_head(key, kv_cols, kv.at[ctx, 0], k_send, k_recv, d))
            sends.append(to_head(value, kv_cols, kv.at[ctx, 1], v_send, v_recv, d))
        for d in some:
            sends.append(to_head(query, q_cols, qbuf, q_send, q_recv, d))
    for copy in sends:
        copy.start()

    def arrived(dst, recv, s):
        pltpu.make_async_copy(dst.at[rows_of(s)], dst.at[rows_of(s)], recv.at[s]).wait()

    def piece_ref(c, p):
        return kv.at[c, :, pl.ds(pl.multiple_of(p * piece_rows, piece_rows), piece_rows)]

    def forward(c, p, dest, send):
        return pltpu.make_async_remote_copy(
            src_ref=piece_ref(c, p), dst_ref=piece_ref(c, p),
            send_sem=send, recv_sem=f_recv.at[c, p],
            device_id={"ctx": dest}, device_id_type=MESH,
        )

    def piece_arrived(c, p):
        pltpu.make_async_copy(piece_ref(c, p), piece_ref(c, p), f_recv.at[c, p]).wait()

    passed = []

    def relay(p):
        for c in same_core:
            piece_arrived(c, p)
            copy = forward(c, p, partner, r_send.at[c, p])
            copy.start()
            passed.append(copy)

    home = me // pair
    near_pieces = pieces // 2
    near_half = home // near_pieces

    def collect(step):
        p = flip(home, step, pieces)
        for t in range(pair):
            s = flip(me, step * pair + t, n_head)
            if step == 0 and t == 0:
                mine[0].wait()
                mine[1].wait()
            else:
                arrived(kv.at[ctx, 0], k_recv, s)
                arrived(kv.at[ctx, 1], v_recv, s)
        for dest in same_core + [partner]:
            copy = forward(ctx, p, dest, f_send.at[dest, p])
            copy.start()
            passed.append(copy)

    def others_arrived(t, steps):
        c = ((chip + t) % chips) * 2 + 1 - core
        for step in steps:
            piece_arrived(c, flip(home, step, pieces))

    ones = jnp.ones((2 * block, HEAD_WIDTH), jnp.bfloat16)

    def unit(step, far, t, diagonal):
        g = flip(home, step, pieces)
        first_row = g * piece_rows
        q_half = first_row // block
        q_block = order[2 * ctx + q_half]
        half = near_half + far - 2 * near_half * far
        c0 = ((chip + t) % chips) * 2 + core
        c1 = ((chip + t) % chips) * 2 + 1 - core
        q_span = pl.ds(pl.multiple_of(first_row, piece_rows), piece_rows)
        k_span = pl.ds(pl.multiple_of(half * block, block), block)
        low = jnp.where(order[2 * c0 + half] <= q_block, 0.0, HIDDEN)
        high = jnp.where(order[2 * c1 + half] <= q_block, 0.0, HIDDEN)
        for h in range(kv_heads):
            cols = slice(h * HEAD_WIDTH, (h + 1) * HEAD_WIDTH)
            q = jnp.concatenate(
                [qbuf[q_span, (h * per_kv + i) * HEAD_WIDTH : (h * per_kv + i + 1) * HEAD_WIDTH] for i in range(per_kv)],
                axis=0,
            )
            k = jnp.concatenate([kv[c0, 0, k_span, cols], kv[c1, 0, k_span, cols]], axis=0)
            v = jnp.concatenate([kv[c0, 1, k_span, cols], kv[c1, 1, k_span, cols]], axis=0)
            x = lax.dot_general(q, k, (((1,), (1,)), ((), ())), preferred_element_type=jnp.float32)
            x = jnp.tanh(x * IN_SCALE) * OUT_SCALE
            if diagonal:
                q_at = first_row - q_half * block + lax.broadcasted_iota(jnp.int32, (piece_rows, block), 0)
                visible = lax.broadcasted_iota(jnp.int32, (piece_rows, block), 1) <= q_at
                e = jnp.exp2(x[:, :block]).reshape(per_kv, piece_rows, block)
                left = jnp.where(visible[None], e, 0.0).reshape(per_kv * piece_rows, block)
            else:
                left = jnp.exp2(x[:, :block] + low)
            w = jnp.concatenate([left, jnp.exp2(x[:, block:] + high)], axis=1).astype(jnp.bfloat16)
            o = jnp.dot(w, jnp.concatenate([v, ones], axis=1), preferred_element_type=jnp.float32)
            if diagonal:
                acc[step, h] = o
            else:
                acc[step, h] += o

    def q_arrived(step):
        for t in range(pair):
            j = step * pair + t

            @pl.when(j > 0)
            def _():
                arrived(qbuf, q_recv, flip(me, j, n_head))

    def finish(step):
        first_row = flip(home, step, pieces) * piece_rows
        span = pl.ds(pl.multiple_of(first_row, piece_rows), piece_rows)
        for h in range(kv_heads):
            a = acc[step, h]
            o = (a[:, :HEAD_WIDTH] / a[:, HEAD_WIDTH:]).astype(jnp.bfloat16)
            for i in range(per_kv):
                at = (h * per_kv + i) * HEAD_WIDTH
                out[span, at : at + HEAD_WIDTH] = o[i * piece_rows : (i + 1) * piece_rows]

    def each(count, body):
        lax.fori_loop(0, count, lambda i, carry: (body(i), carry)[1], 0)

    near_steps, far_steps = range(near_pieces), range(near_pieces, pieces)
    for step in near_steps:
        collect(step)
    for step in near_steps:
        relay(flip(home, step, pieces))
    mine[2].wait()
    for t in range(chips):
        others_arrived(t, near_steps)

    def near_near(step):
        q_arrived(step)
        unit(step, 0, 0, True)
        each(chips - 1, lambda t: unit(step, 0, t + 1, False))

    each(near_pieces, near_near)
    for step in far_steps:
        collect(step)
        if step > near_pieces:
            relay(flip(home, step - 1, pieces))
    others_arrived(0, far_steps)
    each(near_pieces, lambda step: unit(step, 1, 0, False))
    relay(flip(home, pieces - 1, pieces))
    for t in range(1, chips):
        others_arrived(t, far_steps)

    def rest(step):
        each(chips - 1, lambda t: unit(step, 1, t + 1, False))
        finish(step)

    each(near_pieces, rest)

    def far_all(i):
        step = near_pieces + i
        q_arrived(step)
        unit(step, 1, 0, True)
        each(2 * chips - 1, lambda u: unit(step, u // chips, u % chips + u // chips, False))
        finish(step)

    each(near_pieces, far_all)
    for copy in sends:
        copy.wait_send()
    for copy in passed:
        copy.wait_send()


def shards(n_head, n_ctx, query, key, value, block_order):
    rows = query.shape[0]
    total = rows * n_head
    q_cols = query.shape[1] // n_head
    kv_cols = key.shape[1] // n_head
    kv_heads = kv_cols // HEAD_WIDTH
    per_kv = q_cols // kv_cols
    pair = 2
    pieces = n_head // pair
    hbm = pl.BlockSpec(memory_space=pltpu.HBM)
    dma = pltpu.SemaphoreType.DMA
    return pl.pallas_call(
        functools.partial(kernel, n_head, n_ctx, pair),
        out_shape=jax.ShapeDtypeStruct((total, q_cols), jnp.bfloat16),
        in_specs=[pl.BlockSpec(memory_space=pltpu.SMEM), hbm, hbm, hbm],
        out_specs=pl.BlockSpec(memory_space=pltpu.VMEM),
        scratch_shapes=[
            pltpu.VMEM((total, q_cols), jnp.bfloat16),
            pltpu.VMEM((n_ctx, 2, total, kv_cols), jnp.bfloat16),
            pltpu.VMEM((pieces, kv_heads, per_kv * pair * rows, 2 * HEAD_WIDTH), jnp.float32),
            dma((n_head,)), dma((n_head,)), dma((n_head,)),
            dma((n_head,)), dma((n_head,)), dma((n_head,)),
            dma((3,)),
            dma((n_ctx, pieces)), dma((n_ctx, pieces)), dma((n_ctx, pieces)),
        ],
        compiler_params=pltpu.CompilerParams(
            collective_id=0, has_side_effects=True, vmem_limit_bytes=60 * 1024 * 1024
        ),
    )(block_order, query, key, value)


def solution(mesh):
    placed = (P(("ctx", "head"), None), P(("ctx", "head"), None), P(("ctx", "head"), None), P())
    return jax.shard_map(
        functools.partial(shards, mesh.shape["head"], mesh.shape["ctx"]),
        mesh=mesh, in_specs=placed, out_specs=P("ctx", "head"), check_vma=False,
    )
```
